32 devices in a mesh: gx: 2 (over core), gy: 4 (over y, x), gz: 4 (over z).
Axes of the slice: x: 2, y: 2, z: 4, core: 2. Of those that a mesh axis runs over, the one named last changes fastest.
Arguments:
- queries: bfloat16 [128, 32, 128], P(None, 'gy'), may hold values from -6 to 6
- passages: bfloat16 [1024, 256, 128], P('gx', 'gz'), may hold values from -0.5 to 0.5
- passage_len: int32 [1024], P('gx'), may hold values from 32 to 256
- query_len: int32 [128], replicated, may hold values from 8 to 32
Outputs:
- log_probs: float32 [128, 1024], P(None, ('gx', 'gz'))
The draws below stay inside these ranges and needn't reach their ends.
All inputs are finite; a program needn't handle non-finite values.
Results may differ from the reference program's by a relative error of at most 0.0003.
Values sent between devices are 32-bit elements; how exact they have to be, the bound alone decides.
No kernel may reach another device: no remote copies, remote signals or barrier semaphores. Data moves between devices by JAX's collectives and lax.ppermute only.
A program may use at most 64 MiB of HBM per device.

```python
import math
import jax
import jax.numpy as jnp
from jax import lax

DIM = 128
NQ = 128
LQ = 32
LP = 256
NP = 1024


def draw_queries(key, part):
    noise_key = jax.random.fold_in(key, 11)
    values = jnp.clip(jax.random.normal(noise_key, (NQ, LQ, DIM), jnp.float32), -6.0, 6.0)
    return values.astype(jnp.bfloat16)


def draw_passages(key, part):
    noise_key = jax.random.fold_in(key, 21)
    values = jax.random.normal(noise_key, (NP, LP, DIM), jnp.float32) * DIM ** (-0.5)
    values = jnp.clip(values, -0.5, 0.5)
    return values.astype(jnp.bfloat16)


def set_ends(entries, stream_key, smallest, high):
    spot = [jax.random.randint(jax.random.fold_in(stream_key, axis), (), 0, length) for axis, length in enumerate(entries.shape)]
    main_axis = entries.shape.index(max(entries.shape))
    beside = spot[:main_axis] + [(spot[main_axis] + 1) % entries.shape[main_axis]] + spot[main_axis + 1:]
    return entries.at[tuple(spot)].set(smallest).at[tuple(beside)].set(high)


def setup_inputs(seed: int = 0) -> dict:
    arg_keys = jax.random.split(jax.random.key(seed), 5)
    queries = draw_queries(jax.random.fold_in(arg_keys[4], 71), 0)
    passages = draw_passages(jax.random.fold_in(arg_keys[4], 71), 0)
    passage_len = set_ends(jax.random.randint(arg_keys[2], (NP,), LP // 8, LP + 1), jax.random.fold_in(arg_keys[2], 1), LP // 8, LP).astype(jnp.int32)
    query_len = set_ends(jax.random.randint(arg_keys[3], (NQ,), max(1, LQ // 4), LQ + 1), jax.random.fold_in(arg_keys[3], 1), max(1, LQ // 4), LQ).astype(jnp.int32)
    return dict(queries=queries, passages=passages, passage_len=passage_len, query_len=query_len)


masked_low = -1.0e30


def reference(queries, passages, passage_len, query_len):
    flat_queries = queries.reshape(NQ * LQ, DIM)
    per_block = math.gcd(NP, 32)
    num_blocks = NP // per_block
    tile_stack = passages.reshape(num_blocks, per_block * LP, DIM)
    length_stack = passage_len.reshape(num_blocks, per_block)
    query_used = jnp.arange(LQ, dtype=jnp.int32)[None, :] < query_len[:, None]
    token_ids = jnp.arange(LP, dtype=jnp.int32)

    def block_scores(packed):
        passage_tile, tile_len = packed
        scores = jnp.dot(flat_queries, passage_tile.T, preferred_element_type=jnp.float32)
        scores = scores.reshape(NQ * LQ, per_block, LP)
        usable = token_ids[None, :] < tile_len[:, None]
        scores = jnp.where(usable[None], scores, masked_low)
        maxima = jnp.max(scores, axis=2).reshape(NQ, LQ, per_block)
        return jnp.sum(jnp.where(query_used[:, :, None], maxima, 0.0), axis=1)

    pieces = lax.map(block_scores, (tile_stack, length_stack))
    maxsim = jnp.transpose(pieces, (1, 0, 2)).reshape(NQ, NP)
    highest = jnp.max(maxsim, axis=1, keepdims=True)
    summed = jnp.sum(jnp.exp(maxsim - highest), axis=1, keepdims=True)
    return maxsim - (highest + jnp.log(summed))
```

```python
import functools

import jax
import jax.numpy as jnp
from jax import lax
from jax.experimental import pallas as pl
from jax.experimental.pallas import tpu as pltpu
from jax.sharding import PartitionSpec as P

masked_low = -1e30


def maxima_kernel(start_ref, len_ref, queries_ref, passages_ref, out_ref, *, rows_at_once, columns):
    passage_block, token_count, width = passages_ref.shape
    query_rows = queries_ref.shape[0]
    per_dot = rows_at_once // token_count
    first = start_ref[0] + pl.program_id(0) * passage_block
    token_ids = lax.broadcasted_iota(jnp.int32, (token_count, columns), 0)
    for m in range(passage_block // per_dot):
        tile = passages_ref[m * per_dot : (m + 1) * per_dot].reshape(per_dot * token_count, width)
        for j in range(query_rows // columns):
            scores = lax.dot_general(
                tile,
                queries_ref[j * columns : (j + 1) * columns],
                (((1,), (1,)), ((), ())),
                preferred_element_type=jnp.float32,
            )
            best = []
            for k in range(per_dot):
                usable = token_ids < len_ref[first + m * per_dot + k]
                mine = jnp.where(usable, scores[k * token_count : (k + 1) * token_count], masked_low)
                best.append(jnp.max(mine, axis=0, keepdims=True))
            out_ref[m * per_dot : (m + 1) * per_dot, j * columns : (j + 1) * columns] = (
                jnp.concatenate(best, axis=0)
            )


def block_maxima(flat_queries, passages, usable_tokens, block, block_size):
    passage_count, token_count, width = passages.shape
    query_rows = flat_queries.shape[0]
    step = min(64, block_size)
    steps = block_size // step
    return pl.pallas_call(
        functools.partial(
            maxima_kernel,
            rows_at_once=min(step, max(1, 1024 // token_count)) * token_count,
            columns=min(256, query_rows),
        ),
        grid_spec=pltpu.PrefetchScalarGridSpec(
            num_scalar_prefetch=2,
            grid=(steps,),
            in_specs=[
                pl.BlockSpec((query_rows, width), lambda i, start, lens: (0, 0)),
                pl.BlockSpec(
                    (step, token_count, width), lambda i, start, lens: (start[0] // step + i, 0, 0)
                ),
            ],
            out_specs=pl.BlockSpec((step, query_rows), lambda i, start, lens: (i, 0)),
        ),
        out_shape=jax.ShapeDtypeStruct((block_size, query_rows), jnp.float32),
        cost_estimate=pl.CostEstimate(
            flops=2 * 2 * block_size * token_count * query_rows * width,
            bytes_accessed=block_size * (token_count * width * 2 + query_rows * 4),
            transcendentals=0,
        ),
        name="maxima",
    )((block * block_size).reshape(1), usable_tokens, flat_queries, passages)


def exchange(array, axis, distance):
    size = lax.axis_size(axis)
    return lax.ppermute(array, axis, [(k, k ^ distance) for k in range(size)])


def hypercube(array, axis, combine):
    distance = 1
    while distance < lax.axis_size(axis):
        array = combine(array, exchange(array, axis, distance))
        distance *= 2
    return array


def join_pairs(one, other):
    top = jnp.maximum(one[0], other[0])
    summed = one[1] * jnp.exp(one[0] - top) + other[1] * jnp.exp(other[0] - top)
    return jnp.stack([top, summed])


def shards(queries, passages, passage_len, query_len):
    query_count, query_rows, width = queries.shape
    passage_count, token_count, _ = passages.shape
    gz = lax.axis_index("gz")
    owners = lax.axis_size("gz")
    block_size = passage_count // owners
    flat_queries = jnp.transpose(queries, (1, 0, 2)).reshape(query_rows * query_count, width)
    usable_tokens = passage_len - gz * token_count

    merged = None
    arrived = []
    for distance in range(owners - 1, -1, -1):
        block = block_maxima(flat_queries, passages, usable_tokens, gz ^ distance, block_size)
        arrived.append(exchange(block, "gz", distance) if distance else block)
    merged = functools.reduce(jnp.maximum, arrived)
    query_ids = lax.axis_index("gy") * query_rows + jnp.arange(query_rows, dtype=jnp.int32)
    counted = query_ids[:, None] < query_len[None, :]
    partial_value = jnp.sum(
        jnp.where(counted[None], merged.reshape(block_size, query_rows, query_count), 0.0), axis=1
    )
    scores = hypercube(partial_value, "gy", jnp.add)
    top = jnp.max(scores, axis=0)
    summed = jnp.sum(jnp.exp(scores - top[None]), axis=0)
    pair = jnp.stack([top, summed])
    pair = hypercube(pair, "gx", join_pairs)
    pair = hypercube(pair, "gz", join_pairs)
    return jnp.transpose(scores - (pair[0] + jnp.log(pair[1]))[None])


def solution(mesh):
    return jax.shard_map(
        shards,
        mesh=mesh,
        in_specs=(P(None, "gy", None), P("gx", "gz", None), P("gx"), P()),
        out_specs=P(None, ("gx", "gz")),
        check_vma=False,
    )
```

```python
import functools

import jax
import jax.numpy as jnp
from jax import lax
from jax.experimental import pallas as pl
from jax.experimental.pallas import tpu as pltpu
from jax.sharding import PartitionSpec as P

masked_low = -1e30
mebibyte = 2**20


def maxima_kernel(len_ref, queries_ref, passages_ref, out_ref, *, distance, block_size, offset, rows, columns):
    _, token_count, width = passages_ref.shape
    passage_count, query_rows = out_ref.shape
    per_dot = rows // token_count
    gz = lax.axis_index("gz")
    first = (gz ^ distance) * block_size + offset
    hidden = gz * token_count
    token_ids = lax.broadcasted_iota(jnp.int32, (token_count, columns), 0)
    for m in range(passage_count // per_dot):
        tile = passages_ref[pl.ds(first + m * per_dot, per_dot)].reshape(rows, width)
        for j in range(query_rows // columns):
            scores = lax.dot_general(
                tile,
                queries_ref[j * columns : (j + 1) * columns],
                (((1,), (1,)), ((), ())),
                preferred_element_type=jnp.float32,
            )
            best = []
            for k in range(per_dot):
                usable = token_ids < len_ref[first + m * per_dot + k] - hidden
                mine = jnp.where(usable, scores[k * token_count : (k + 1) * token_count], masked_low)
                best.append(jnp.max(mine, axis=0, keepdims=True))
            out_ref[m * per_dot : (m + 1) * per_dot, j * columns : (j + 1) * columns] = (
                jnp.concatenate(best, axis=0)
            )


def maxima(flat_queries, passages, passage_len, distance, block_size, offset, size):
    _, token_count, width = passages.shape
    query_rows = flat_queries.shape[0]
    per_dot = min(size, max(1, 1024 // token_count))
    return pl.pallas_call(
        functools.partial(
            maxima_kernel,
            distance=distance,
            block_size=block_size,
            offset=offset,
            rows=per_dot * token_count,
            columns=min(256, query_rows),
        ),
        in_specs=[
            pl.BlockSpec(memory_space=pltpu.SMEM),
            pl.BlockSpec(memory_space=pltpu.VMEM),
            pl.BlockSpec(memory_space=pltpu.VMEM),
        ],
        out_specs=pl.BlockSpec(memory_space=pltpu.VMEM),
        out_shape=jax.ShapeDtypeStruct((size, query_rows), jnp.float32),
        cost_estimate=pl.CostEstimate(
            flops=2 * 2 * size * token_count * query_rows * width,
            bytes_accessed=size * (token_count * width * 2 + query_rows * 4),
            transcendentals=0,
        ),
        compiler_params=pltpu.CompilerParams(vmem_limit_bytes=12 * mebibyte),
        name=f"maxima_{distance}_{offset}",
    )(passage_len, flat_queries, passages)


def merge_kernel(*refs):
    *part_refs, len_ref, out_ref = refs
    query_count = out_ref.shape[1]
    lanes = part_refs[0].shape[1]
    query_rows = lanes // query_count
    merged = functools.reduce(jnp.maximum, [part[...] for part in part_refs])
    shape = (lanes, query_count)
    row = lax.broadcasted_iota(jnp.int32, shape, 0)
    start = lax.broadcasted_iota(jnp.int32, shape, 1) * query_rows
    used = jnp.clip(len_ref[...] - lax.axis_index("gy") * query_rows, 0, query_rows)
    counted = jnp.where((row >= start) & (row < start + used), 1.0, 0.0).astype(jnp.bfloat16)
    total = None
    for _ in range(3):
        piece = merged.astype(jnp.bfloat16)
        merged = merged - piece.astype(jnp.float32)
        term = jnp.dot(piece, counted, preferred_element_type=jnp.float32)
        total = term if total is None else total + term
    out_ref[...] = total


def merge(parts, query_len):
    query_count = query_len.shape[0]
    block_size = parts[0].shape[0]
    return pl.pallas_call(
        merge_kernel,
        out_shape=jax.ShapeDtypeStruct((block_size, query_count), jnp.float32),
        compiler_params=pltpu.CompilerParams(vmem_limit_bytes=12 * mebibyte),
        name="merge",
    )(*parts, query_len.reshape(1, query_count))


def exchange(array, axis, distance):
    size = lax.axis_size(axis)
    return lax.ppermute(array, axis, [(k, k ^ distance) for k in range(size)])


def hypercube(array, axis, combine):
    distance = 1
    while distance < lax.axis_size(axis):
        array = combine(array, exchange(array, axis, distance))
        distance *= 2
    return array


def join_pairs(one, other):
    top = jnp.maximum(one[0], other[0])
    summed = one[1] * jnp.exp(one[0] - top) + other[1] * jnp.exp(other[0] - top)
    return jnp.stack([top, summed])


def owned_maxima(score, block_size, owners):
    if owners != 4:
        return [
            exchange(score(distance, 0, block_size), "gz", distance) if distance else score(0, 0, block_size)
            for distance in range(owners - 1, -1, -1)
        ]
    half = block_size // 2
    near = [exchange(score(3, part * half, half), "gz", 1) for part in range(2)]
    far = []
    for part in range(2):
        joined = jnp.maximum(score(2, part * half, half), near[part])
        far.append(exchange(joined, "gz", 2))
    beside = exchange(score(1, 0, block_size), "gz", 1)
    return [score(0, 0, block_size), beside, jnp.concatenate(far)]


def shards(queries, passages, passage_len, query_len):
    query_count, query_rows, width = queries.shape
    passage_count = passages.shape[0]
    owners = lax.axis_size("gz")
    block_size = passage_count // owners
    flat_queries = queries.reshape(query_count * query_rows, width)
    held = pltpu.with_memory_space_constraint(passages, pltpu.VMEM)

    def score(distance, offset, size):
        return maxima(flat_queries, held, passage_len, distance, block_size, offset, size)

    partial_value = merge(owned_maxima(score, block_size, owners), query_len)
    scores = hypercube(partial_value, "gy", jnp.add)
    top = jnp.max(scores, axis=0)
    summed = jnp.sum(jnp.exp(scores - top[None]), axis=0)
    pair = hypercube(jnp.stack([top, summed]), "gx", join_pairs)
    pair = hypercube(pair, "gz", join_pairs)
    return jnp.transpose(scores - (pair[0] + jnp.log(pair[1]))[None])


def solution(mesh):
    return jax.shard_map(
        shards,
        mesh=mesh,
        in_specs=(P(None, "gy", None), P("gx", "gz", None), P("gx"), P()),
        out_specs=P(None, ("gx", "gz")),
        check_vma=False,
    )
```

```python
import functools

import jax
import jax.numpy as jnp
from jax import lax
from jax.experimental import pallas as pl
from jax.experimental.pallas import tpu as pltpu
from jax.sharding import PartitionSpec as P


masked_low = -1e30
mebibyte = 2**20


def best_tokens(len_ref, queries_ref, passages_ref, out_ref, first, place, rows, columns):
    _, token_count, width = passages_ref.shape
    query_rows = out_ref.shape[1]
    per_dot = rows // token_count
    hidden = lax.axis_index("gz") * token_count
    token_ids = lax.broadcasted_iota(jnp.int32, (token_count, columns), 0)
    tile = passages_ref[pl.ds(first, per_dot)].reshape(rows, width)
    for j in range(query_rows // columns):
        scores = lax.dot_general(
            tile,
            queries_ref[j * columns : (j + 1) * columns],
            (((1,), (1,)), ((), ())),
            preferred_element_type=jnp.float32,
        )
        best = []
        for k in range(per_dot):
            usable = token_ids < len_ref[first + k] - hidden
            mine = jnp.where(usable, scores[k * token_count : (k + 1) * token_count], masked_low)
            best.append(jnp.max(mine, axis=0, keepdims=True))
        out_ref[place : place + per_dot, j * columns : (j + 1) * columns] = jnp.concatenate(best, axis=0)


def first_kernel(
    len_hbm, queries_hbm, passages_hbm, out_ref, len_out, queries_ref, passages_ref, sems,
    *, distance, block_size, rows, columns
):
    passage_count, token_count, _ = passages_hbm.shape
    size = out_ref.shape[0]
    per_dot = rows // token_count
    first = (lax.axis_index("gz") ^ distance) * block_size
    copies = [
        pltpu.make_async_copy(len_hbm, len_out, sems.at[0]),
        pltpu.make_async_copy(queries_hbm, queries_ref, sems.at[1]),
    ]
    for m in range(passage_count // per_dot):
        place = lax.rem(first + m * per_dot, passage_count)
        copies.append(
            pltpu.make_async_copy(
                passages_hbm.at[pl.ds(place, per_dot)], passages_ref.at[pl.ds(place, per_dot)], sems.at[2 + m]
            )
        )
    for copy in copies:
        copy.start()
    copies[0].wait()
    copies[1].wait()
    for m in range(size // per_dot):
        copies[2 + m].wait()
        best_tokens(
            len_out, queries_ref, passages_ref, out_ref, first + m * per_dot, m * per_dot, rows, columns
        )
    for copy in copies[2 + size // per_dot :]:
        copy.wait()


def maxima_kernel(len_ref, queries_ref, passages_ref, out_ref, *, distance, block_size, offset, rows, columns):
    first = (lax.axis_index("gz") ^ distance) * block_size + offset
    per_dot = rows // passages_ref.shape[1]
    for m in range(out_ref.shape[0] // per_dot):
        best_tokens(
            len_ref, queries_ref, passages_ref, out_ref, first + m * per_dot, m * per_dot, rows, columns
        )


def maxima(flat_queries, passages, passage_len, distance, block_size, offset, size, fill=False):
    passage_count, token_count, width = passages.shape
    query_rows = flat_queries.shape[0]
    per_dot = min(size, max(1, 1024 // token_count))
    settings = dict(
        distance=distance,
        block_size=block_size,
        rows=per_dot * token_count,
        columns=min(256, query_rows),
    )
    result = jax.ShapeDtypeStruct((size, query_rows), jnp.float32)
    smem, vmem = pl.BlockSpec(memory_space=pltpu.SMEM), pl.BlockSpec(memory_space=pltpu.VMEM)
    common = dict(
        cost_estimate=pl.CostEstimate(
            flops=2 * 2 * size * token_count * query_rows * width,
            bytes_accessed=size * (token_count * width * 2 + query_rows * 4),
            transcendentals=0,
        ),
        compiler_params=pltpu.CompilerParams(vmem_limit_bytes=14 * mebibyte),
        name=f"maxima_{distance}_{offset}",
    )
    operands = (passage_len, flat_queries, passages)
    if fill:
        return pl.pallas_call(
            functools.partial(first_kernel, **settings),
            in_specs=[pl.BlockSpec(memory_space=pltpu.HBM)] * 3,
            out_specs=[vmem, smem, vmem, vmem],
            out_shape=[result, *(jax.ShapeDtypeStruct(x.shape, x.dtype) for x in operands)],
            scratch_shapes=[pltpu.SemaphoreType.DMA((2 + passage_count // per_dot,))],
            **common,
        )(*operands)
    return pl.pallas_call(
        functools.partial(maxima_kernel, offset=offset, **settings),
        in_specs=[smem, vmem, vmem],
        out_specs=vmem,
        out_shape=result,
        **common,
    )(*operands)


def merge_kernel(*refs):
    *part_refs, len_ref, out_ref = refs
    query_count = out_ref.shape[1]
    lanes = part_refs[0].shape[1]
    query_rows = lanes // query_count
    merged = functools.reduce(jnp.maximum, [part[...] for part in part_refs])
    shape = (lanes, query_count)
    row = lax.broadcasted_iota(jnp.int32, shape, 0)
    start = lax.broadcasted_iota(jnp.int32, shape, 1) * query_rows
    used = jnp.clip(len_ref[...] - lax.axis_index("gy") * query_rows, 0, query_rows)
    counted = jnp.where((row >= start) & (row < start + used), 1.0, 0.0).astype(jnp.bfloat16)
    total = None
    for _ in range(3):
        piece = merged.astype(jnp.bfloat16)
        merged = merged - piece.astype(jnp.float32)
        term = jnp.dot(piece, counted, preferred_element_type=jnp.float32)
        total = term if total is None else total + term
    out_ref[...] = total


def merge(parts, query_len):
    query_count = query_len.shape[0]
    block_size = parts[0].shape[0]
    return pl.pallas_call(
        merge_kernel,
        out_shape=jax.ShapeDtypeStruct((block_size, query_count), jnp.float32),
        compiler_params=pltpu.CompilerParams(vmem_limit_bytes=12 * mebibyte),
        name="merge",
    )(*parts, query_len.reshape(1, query_count))


def exchange(array, axis, distance):
    size = lax.axis_size(axis)
    return lax.ppermute(array, axis, [(k, k ^ distance) for k in range(size)])


def hypercube(array, axis, combine):
    distance = 1
    while distance < lax.axis_size(axis):
        array = combine(array, exchange(array, axis, distance))
        distance *= 2
    return array


def join_pairs(one, other):
    top = jnp.maximum(one[0], other[0])
    summed = one[1] * jnp.exp(one[0] - top) + other[1] * jnp.exp(other[0] - top)
    return jnp.stack([top, summed])


def owned_maxima(score, start, block_size, owners):
    if owners != 4:
        size = start.shape[0]
        rest = [score(owners - 1, size, block_size - size)] if size < block_size else []
        sent = jnp.concatenate([start, *rest])
        return [exchange(sent, "gz", owners - 1)] + [
            exchange(score(distance, 0, block_size), "gz", distance) if distance else score(0, 0, block_size)
            for distance in range(owners - 2, -1, -1)
        ]
    half = start.shape[0]
    rest = block_size - half
    near = [named_exchange(start, 1), named_exchange(score(3, half, rest), 1)]
    far_0 = named_exchange(jnp.maximum(score(2, 0, half), near[0]), 2)
    beside = named_exchange(score(1, 0, block_size), 1)
    far_1 = named_exchange(jnp.maximum(score(2, half, rest), near[1]), 2)
    return [score(0, 0, block_size), beside, jnp.concatenate([far_0, far_1])]


def named_exchange(array, distance):
    return exchange(array, "gz", distance)


def shards(queries, passages, passage_len, query_len):
    query_count, query_rows, width = queries.shape
    passage_count = passages.shape[0]
    owners = lax.axis_size("gz")
    block_size = passage_count // owners
    flat_queries = queries.reshape(query_count * query_rows, width)
    flat_queries, passages, passage_len = (
        pltpu.with_memory_space_constraint(x, pltpu.HBM) for x in (flat_queries, passages, passage_len)
    )
    start, lengths, held_queries, held = maxima(
        flat_queries, passages, passage_len, owners - 1, block_size, 0, block_size // 2, fill=True
    )
    held = pltpu.with_memory_space_constraint(held, pltpu.VMEM)
    held_queries = pltpu.with_memory_space_constraint(held_queries, pltpu.VMEM)

    def score(distance, offset, size):
        return maxima(held_queries, held, lengths, distance, block_size, offset, size)

    partial_value = merge(owned_maxima(score, start, block_size, owners), query_len)
    scores = hypercube(partial_value, "gy", jnp.add)
    top = jnp.max(scores, axis=0)
    summed = jnp.sum(jnp.exp(scores - top[None]), axis=0)
    pair = hypercube(jnp.stack([top, summed]), "gx", join_pairs)
    pair = hypercube(pair, "gz", join_pairs)
    return jnp.transpose(scores - (pair[0] + jnp.log(pair[1]))[None])


def solution(mesh):
    return jax.shard_map(
        shards,
        mesh=mesh,
        in_specs=(P(None, "gy", None), P("gx", "gz", None), P("gx"), P()),
        out_specs=P(None, ("gx", "gz")),
        check_vma=False,
    )
```

```python
import functools

import jax
import jax.numpy as jnp
from jax import lax
from jax.experimental import pallas as pl
from jax.experimental.pallas import tpu as pltpu
from jax.sharding import PartitionSpec as P


masked_low = -1e30
mebibyte = 2**20


def best_tokens(len_ref, queries_ref, passages_ref, out_ref, first_len, first, place, per_dot, columns):
    _, token_count, width = passages_ref.shape
    query_rows = out_ref.shape[1]
    hidden = lax.axis_index("gz") * token_count
    token_ids = lax.broadcasted_iota(jnp.int32, (token_count, columns), 0)
    tile = passages_ref[first : first + per_dot].reshape(per_dot * token_count, width)
    for j in range(query_rows // columns):
        scores = lax.dot_general(
            tile,
            queries_ref[j * columns : (j + 1) * columns],
            (((1,), (1,)), ((), ())),
            preferred_element_type=jnp.float32,
        )
        best = []
        for k in range(per_dot):
            usable = token_ids < len_ref[first_len + k] - hidden
            mine = jnp.where(usable, scores[k * token_count : (k + 1) * token_count], masked_low)
            best.append(jnp.max(mine, axis=0, keepdims=True))
        out_ref[place : place + per_dot, j * columns : (j + 1) * columns] = jnp.concatenate(best, axis=0)


def block_copies(passages_hbm, block_ref, sems, distance, per_copy):
    block_size = block_ref.shape[0]
    first = (lax.axis_index("gz") ^ distance) * block_size
    return [
        pltpu.make_async_copy(
            passages_hbm.at[pl.ds(first + place, per_copy)],
            block_ref.at[pl.ds(place, per_copy)],
            sems.at[place // per_copy],
        )
        for place in range(0, block_size, per_copy)
    ]


def start_all(passages_hbm, block_ref, sems, distance, per_copy):
    block_size = block_ref.shape[0]
    first = (lax.axis_index("gz") ^ distance) * block_size

    @pl.loop(0, block_size // per_copy)
    def _(m):
        place = m * per_copy
        pltpu.make_async_copy(
            passages_hbm.at[pl.ds(first + place, per_copy)],
            block_ref.at[pl.ds(place, per_copy)],
            sems.at[m],
        ).start()


def first_kernel(
    len_hbm, queries_hbm, passages_hbm, out_ref, len_ref, queries_ref, block_ref, own_sems, sems,
    *, distance, per_dot, columns
):
    own = [
        pltpu.make_async_copy(queries_hbm, queries_ref, own_sems.at[0]),
        pltpu.make_async_copy(len_hbm, len_ref, own_sems.at[1]),
    ]
    copies = block_copies(passages_hbm, block_ref, sems, distance, per_dot)
    done = out_ref.shape[0] // per_dot
    for copy in own + copies[:done]:
        copy.start()
    for copy in own:
        copy.wait()
    first_len = (lax.axis_index("gz") ^ distance) * block_ref.shape[0]
    for m in range(done):
        copies[m].wait()
        if m == 0:
            for copy in copies[done:]:
                copy.start()
        place = m * per_dot
        best_tokens(
            len_ref, queries_ref, block_ref, out_ref, first_len + place, place, place, per_dot, columns
        )
    for copy in copies[done:]:
        copy.wait()


def maxima_kernel(*refs, distance, offset, ahead, per_dot, columns):
    if ahead is None:
        len_ref, queries_ref, block_ref, out_ref = refs
        copies = []
    else:
        len_ref, queries_ref, block_ref, passages_hbm, out_ref, ahead_ref, sems = refs
        copies = block_copies(passages_hbm, ahead_ref, sems, ahead, per_dot)
        start_all(passages_hbm, ahead_ref, sems, ahead, per_dot)
    first_len = (lax.axis_index("gz") ^ distance) * block_ref.shape[0] + offset
    for place in range(0, out_ref.shape[0], per_dot):
        best_tokens(
            len_ref, queries_ref, block_ref, out_ref, first_len + place, offset + place, place, per_dot, columns
        )
    for copy in copies:
        copy.wait()


class Scorer:
    def __init__(self, queries, passages, passage_len, owners):
        self.arguments = [
            pltpu.with_memory_space_constraint(x, pltpu.HBM) for x in (passage_len, queries, passages)
        ]
        passage_count, self.token_count, self.width = passages.shape
        self.query_rows = queries.shape[0]
        self.block_shape = (passage_count // owners, self.token_count, self.width)
        self.block_type = jax.ShapeDtypeStruct(self.block_shape, passages.dtype)
        self.on_chip = {}

    def settings(self, distance, offset, size):
        per_dot = min(16, max(1, 1024 // self.token_count))
        while size % per_dot or self.block_shape[0] % per_dot:
            per_dot //= 2
        fixed = dict(
            out_specs=pl.BlockSpec(memory_space=pltpu.VMEM),
            cost_estimate=pl.CostEstimate(
                flops=4 * size * self.token_count * self.query_rows * self.width,
                bytes_accessed=size * (self.token_count * self.width * 2 + self.query_rows * 4),
                transcendentals=0,
            ),
            compiler_params=pltpu.CompilerParams(vmem_limit_bytes=12 * mebibyte),
            name=f"maxima_{distance}_{offset}",
        )
        result = jax.ShapeDtypeStruct((size, self.query_rows), jnp.float32)
        return per_dot, min(256, self.query_rows), fixed, result

    def first(self, distance, size):
        per_dot, columns, fixed, result = self.settings(distance, 0, size)
        vmem = fixed.pop("out_specs")
        lengths, queries, _ = self.arguments
        start, self.lengths, self.queries, block = pl.pallas_call(
            functools.partial(first_kernel, distance=distance, per_dot=per_dot, columns=columns),
            in_specs=[pl.BlockSpec(memory_space=pltpu.HBM)] * 3,
            out_specs=[vmem, pl.BlockSpec(memory_space=pltpu.SMEM), vmem, vmem],
            out_shape=[
                result,
                jax.ShapeDtypeStruct(lengths.shape, lengths.dtype),
                jax.ShapeDtypeStruct(queries.shape, queries.dtype),
                self.block_type,
            ],
            scratch_shapes=[
                pltpu.SemaphoreType.DMA((2,)),
                pltpu.SemaphoreType.DMA((self.block_shape[0] // per_dot,)),
            ],
            **fixed,
        )(*self.arguments)
        self.queries = pltpu.with_memory_space_constraint(self.queries, pltpu.VMEM)
        self.on_chip[distance] = pltpu.with_memory_space_constraint(block, pltpu.VMEM)
        return start

    def __call__(self, distance, offset, size, ahead=None):
        per_dot, columns, fixed, result = self.settings(distance, offset, size)
        vmem = fixed.pop("out_specs")
        in_specs = [pl.BlockSpec(memory_space=pltpu.SMEM), vmem, vmem]
        operands = [self.lengths, self.queries, self.on_chip[distance]]
        out_specs, out_shape, scratch = [vmem], [result], []
        if ahead is not None:
            in_specs.append(pl.BlockSpec(memory_space=pltpu.HBM))
            operands.append(self.arguments[2])
            out_specs.append(vmem)
            out_shape.append(self.block_type)
            scratch = [pltpu.SemaphoreType.DMA((self.block_shape[0] // per_dot,))]
        maxima, *block = pl.pallas_call(
            functools.partial(
                maxima_kernel,
                distance=distance,
                offset=offset,
                ahead=ahead,
                per_dot=per_dot,
                columns=columns,
            ),
            in_specs=in_specs,
            out_specs=out_specs,
            out_shape=out_shape,
            scratch_shapes=scratch,
            **fixed,
        )(*operands)
        if block:
            self.on_chip[ahead] = pltpu.with_memory_space_constraint(block[0], pltpu.VMEM)
        return maxima


def merge_kernel(*refs, offsets):
    *part_refs, len_ref, out_ref = refs
    size, query_count = out_ref.shape
    lanes = part_refs[0].shape[1]
    query_rows = lanes // query_count
    merged = functools.reduce(
        jnp.maximum, [part[offset : offset + size] for part, offset in zip(part_refs, offsets)]
    )
    shape = (lanes, query_count)
    row = lax.broadcasted_iota(jnp.int32, shape, 0)
    start = lax.broadcasted_iota(jnp.int32, shape, 1) * query_rows
    used = jnp.clip(len_ref[...] - lax.axis_index("gy") * query_rows, 0, query_rows)
    counted = jnp.where((row >= start) & (row < start + used), 1.0, 0.0).astype(jnp.bfloat16)
    total = None
    for _ in range(3):
        piece = merged.astype(jnp.bfloat16)
        merged = merged - piece.astype(jnp.float32)
        term = jnp.dot(piece, counted, preferred_element_type=jnp.float32)
        total = term if total is None else total + term
    out_ref[...] = total


def merge(parts, offsets, size, query_len):
    query_count = query_len.shape[0]
    return pl.pallas_call(
        functools.partial(merge_kernel, offsets=offsets),
        out_shape=jax.ShapeDtypeStruct((size, query_count), jnp.float32),
        compiler_params=pltpu.CompilerParams(vmem_limit_bytes=12 * mebibyte),
    )(*parts, query_len.reshape(1, query_count))


def exchange(array, axis, distance):
    size = lax.axis_size(axis)
    return lax.ppermute(array, axis, [(k, k ^ distance) for k in range(size)])


def hypercube(array, axis, combine):
    distance = 1
    while distance < lax.axis_size(axis):
        array = combine(array, exchange(array, axis, distance))
        distance *= 2
    return array


def join_pairs(one, other):
    top = jnp.maximum(one[0], other[0])
    summed = one[1] * jnp.exp(one[0] - top) + other[1] * jnp.exp(other[0] - top)
    return jnp.stack([top, summed])


def summed_scores(scorer, query_len, owners):
    block_size = scorer.block_shape[0]
    if owners != 4:
        sent = scorer.first(owners - 1, block_size)
        parts = []
        for distance in range(owners - 1, -1, -1):
            ahead = distance - 1 if distance > 0 else None
            if distance < owners - 1:
                sent = scorer(distance, 0, block_size, ahead)
            elif ahead is not None:
                scorer(distance, 0, block_size, ahead)
            parts.append(exchange(sent, "gz", distance) if distance else sent)
        total = merge(parts, [0] * len(parts), block_size, query_len)
        return hypercube(total, "gy", jnp.add)
    early = block_size * 3 // 8
    late = block_size - early
    near_0 = exchange(scorer.first(3, early), "gz", 1)
    near_1 = exchange(scorer(3, early, late, 2), "gz", 1)
    far_0 = exchange(jnp.maximum(scorer(2, 0, early, 1), near_0), "gz", 2)
    beside_0 = exchange(scorer(1, 0, early, 0), "gz", 1)
    far_1 = exchange(jnp.maximum(scorer(2, early, late), near_1), "gz", 2)
    beside_1 = exchange(scorer(1, early, late), "gz", 1)
    own = scorer(0, 0, block_size)
    first = merge([own, beside_0, far_0], [0, 0, 0], early, query_len)
    first = hypercube(first, "gy", jnp.add)
    second = merge([own, beside_1, far_1], [early, 0, 0], late, query_len)
    others = [exchange(second, "gy", distance) for distance in range(1, lax.axis_size("gy"))]
    second = functools.reduce(jnp.add, others, second)
    return jnp.concatenate([first, second])


def shards(queries, passages, passage_len, query_len):
    query_count, query_rows, width = queries.shape
    owners = lax.axis_size("gz")
    flat_queries = queries.reshape(query_count * query_rows, width)
    scorer = Scorer(flat_queries, passages, passage_len, owners)
    scores = summed_scores(scorer, query_len, owners)
    top = jnp.max(scores, axis=0)
    summed = jnp.sum(jnp.exp(scores - top[None]), axis=0)
    pair = hypercube(jnp.stack([top, summed]), "gx", join_pairs)
    others = [exchange(pair, "gz", distance) for distance in range(1, owners)]
    pair = functools.reduce(join_pairs, others, pair)
    return jnp.transpose(scores - (pair[0] + jnp.log(pair[1]))[None])


def solution(mesh):
    return jax.shard_map(
        shards,
        mesh=mesh,
        in_specs=(P(None, "gy", None), P("gx", "gz", None), P("gx"), P()),
        out_specs=P(None, ("gx", "gz")),
        check_vma=False,
    )
```

```python
import functools

import jax
import jax.numpy as jnp
from jax import lax
from jax.experimental import pallas as pl
from jax.experimental.pallas import tpu as pltpu
from jax.sharding import PartitionSpec as P


masked_low = -1e30
mebibyte = 2**20


def best_tokens(len_ref, queries_ref, passages_ref, out_ref, first_len, first, place, per_dot, columns):
    _, token_count, width = passages_ref.shape
    query_rows = out_ref.shape[1]
    hidden = lax.axis_index("gz") * token_count
    token_ids = lax.broadcasted_iota(jnp.int32, (token_count, columns), 0)
    tile = passages_ref[first : first + per_dot].reshape(per_dot * token_count, width)
    for j in range(query_rows // columns):
        scores = lax.dot_general(
            tile,
            queries_ref[j * columns : (j + 1) * columns],
            (((1,), (1,)), ((), ())),
            preferred_element_type=jnp.float32,
        )
        best = []
        for k in range(per_dot):
            usable = token_ids < len_ref[first_len + k] - hidden
            mine = jnp.where(usable, scores[k * token_count : (k + 1) * token_count], masked_low)
            best.append(jnp.max(mine, axis=0, keepdims=True))
        out_ref[place : place + per_dot, j * columns : (j + 1) * columns] = jnp.concatenate(best, axis=0)


def block_copies(passages_hbm, block_ref, sems, distance, per_copy):
    block_size = block_ref.shape[0]
    first = (lax.axis_index("gz") ^ distance) * block_size
    return [
        pltpu.make_async_copy(
            passages_hbm.at[pl.ds(first + place, per_copy)],
            block_ref.at[pl.ds(place, per_copy)],
            sems.at[place // per_copy],
        )
        for place in range(0, block_size, per_copy)
    ]


def start_all(passages_hbm, block_ref, sems, distance, per_copy):
    block_size = block_ref.shape[0]
    first = (lax.axis_index("gz") ^ distance) * block_size

    @pl.loop(0, block_size // per_copy)
    def _(m):
        place = m * per_copy
        pltpu.make_async_copy(
            passages_hbm.at[pl.ds(first + place, per_copy)],
            block_ref.at[pl.ds(place, per_copy)],
            sems.at[m],
        ).start()


def first_kernel(
    len_hbm, queries_hbm, passages_hbm, out_ref, len_ref, queries_ref, block_ref, own_sems, sems,
    *, distance, per_dot, columns
):
    own = [
        pltpu.make_async_copy(queries_hbm, queries_ref, own_sems.at[0]),
        pltpu.make_async_copy(len_hbm, len_ref, own_sems.at[1]),
    ]
    copies = block_copies(passages_hbm, block_ref, sems, distance, per_dot)
    done = out_ref.shape[0] // per_dot
    for copy in own + copies[:done]:
        copy.start()
    for copy in own:
        copy.wait()
    first_len = (lax.axis_index("gz") ^ distance) * block_ref.shape[0]
    for m in range(done):
        copies[m].wait()
        if m == 0:
            for copy in copies[done:]:
                copy.start()
        place = m * per_dot
        best_tokens(
            len_ref, queries_ref, block_ref, out_ref, first_len + place, place, place, per_dot, columns
        )
    for copy in copies[done:]:
        copy.wait()


def maxima_kernel(*refs, distance, offset, ahead, per_dot, columns):
    if ahead is None:
        len_ref, queries_ref, block_ref, out_ref = refs
        copies = []
    else:
        len_ref, queries_ref, block_ref, passages_hbm, out_ref, ahead_ref, sems = refs
        copies = block_copies(passages_hbm, ahead_ref, sems, ahead, per_dot)
        start_all(passages_hbm, ahead_ref, sems, ahead, per_dot)
    first_len = (lax.axis_index("gz") ^ distance) * block_ref.shape[0] + offset
    for place in range(0, out_ref.shape[0], per_dot):
        best_tokens(
            len_ref, queries_ref, block_ref, out_ref, first_len + place, offset + place, place, per_dot, columns
        )
    for copy in copies:
        copy.wait()


class Scorer:
    def __init__(self, queries, passages, passage_len, owners):
        self.arguments = [
            pltpu.with_memory_space_constraint(x, pltpu.HBM) for x in (passage_len, queries, passages)
        ]
        passage_count, self.token_count, self.width = passages.shape
        self.query_rows = queries.shape[0]
        self.block_shape = (passage_count // owners, self.token_count, self.width)
        self.block_type = jax.ShapeDtypeStruct(self.block_shape, passages.dtype)
        self.on_chip = {}

    def settings(self, distance, offset, size):
        per_dot = min(16, max(1, 1024 // self.token_count))
        while size % per_dot or self.block_shape[0] % per_dot:
            per_dot //= 2
        fixed = dict(
            out_specs=pl.BlockSpec(memory_space=pltpu.VMEM),
            cost_estimate=pl.CostEstimate(
                flops=4 * size * self.token_count * self.query_rows * self.width,
                bytes_accessed=size * (self.token_count * self.width * 2 + self.query_rows * 4),
                transcendentals=0,
            ),
            compiler_params=pltpu.CompilerParams(vmem_limit_bytes=12 * mebibyte),
            name=f"maxima_{distance}_{offset}",
        )
        result = jax.ShapeDtypeStruct((size, self.query_rows), jnp.float32)
        return per_dot, min(256, self.query_rows), fixed, result

    def first(self, distance, size):
        per_dot, columns, fixed, result = self.settings(distance, 0, size)
        vmem = fixed.pop("out_specs")
        lengths, queries, _ = self.arguments
        start, self.lengths, self.queries, block = pl.pallas_call(
            functools.partial(first_kernel, distance=distance, per_dot=per_dot, columns=columns),
            in_specs=[pl.BlockSpec(memory_space=pltpu.HBM)] * 3,
            out_specs=[vmem, pl.BlockSpec(memory_space=pltpu.SMEM), vmem, vmem],
            out_shape=[
                result,
                jax.ShapeDtypeStruct(lengths.shape, lengths.dtype),
                jax.ShapeDtypeStruct(queries.shape, queries.dtype),
                self.block_type,
            ],
            scratch_shapes=[
                pltpu.SemaphoreType.DMA((2,)),
                pltpu.SemaphoreType.DMA((self.block_shape[0] // per_dot,)),
            ],
            **fixed,
        )(*self.arguments)
        self.queries = pltpu.with_memory_space_constraint(self.queries, pltpu.VMEM)
        self.on_chip[distance] = pltpu.with_memory_space_constraint(block, pltpu.VMEM)
        return start

    def __call__(self, distance, offset, size, ahead=None):
        per_dot, columns, fixed, result = self.settings(distance, offset, size)
        vmem = fixed.pop("out_specs")
        in_specs = [pl.BlockSpec(memory_space=pltpu.SMEM), vmem, vmem]
        operands = [self.lengths, self.queries, self.on_chip[distance]]
        out_specs, out_shape, scratch = [vmem], [result], []
        if ahead is not None:
            in_specs.append(pl.BlockSpec(memory_space=pltpu.HBM))
            operands.append(self.arguments[2])
            out_specs.append(vmem)
            out_shape.append(self.block_type)
            scratch = [pltpu.SemaphoreType.DMA((self.block_shape[0] // per_dot,))]
        maxima, *block = pl.pallas_call(
            functools.partial(
                maxima_kernel,
                distance=distance,
                offset=offset,
                ahead=ahead,
                per_dot=per_dot,
                columns=columns,
            ),
            in_specs=in_specs,
            out_specs=out_specs,
            out_shape=out_shape,
            scratch_shapes=scratch,
            **fixed,
        )(*operands)
        if block:
            self.on_chip[ahead] = pltpu.with_memory_space_constraint(block[0], pltpu.VMEM)
        return maxima


def merge_kernel(*refs, offsets):
    *part_refs, len_ref, out_ref = refs
    size, query_count = out_ref.shape
    lanes = part_refs[0].shape[1]
    query_rows = lanes // query_count
    merged = functools.reduce(
        jnp.maximum, [part[offset : offset + size] for part, offset in zip(part_refs, offsets)]
    )
    shape = (lanes, query_count)
    row = lax.broadcasted_iota(jnp.int32, shape, 0)
    start = lax.broadcasted_iota(jnp.int32, shape, 1) * query_rows
    used = jnp.clip(len_ref[...] - lax.axis_index("gy") * query_rows, 0, query_rows)
    counted = jnp.where((row >= start) & (row < start + used), 1.0, 0.0).astype(jnp.bfloat16)
    total = None
    for _ in range(3):
        piece = merged.astype(jnp.bfloat16)
        merged = merged - piece.astype(jnp.float32)
        term = jnp.dot(piece, counted, preferred_element_type=jnp.float32)
        total = term if total is None else total + term
    out_ref[...] = total


def merge(parts, offsets, size, query_len):
    query_count = query_len.shape[0]
    return pl.pallas_call(
        functools.partial(merge_kernel, offsets=offsets),
        out_shape=jax.ShapeDtypeStruct((size, query_count), jnp.float32),
        compiler_params=pltpu.CompilerParams(vmem_limit_bytes=12 * mebibyte),
    )(*parts, query_len.reshape(1, query_count))


def exchange(array, axis, distance):
    size = lax.axis_size(axis)
    return lax.ppermute(array, axis, [(k, k ^ distance) for k in range(size)])


def hypercube(array, axis, combine):
    distance = 1
    while distance < lax.axis_size(axis):
        array = combine(array, exchange(array, axis, distance))
        distance *= 2
    return array


def join_pairs(one, other):
    top = jnp.maximum(one[0], other[0])
    summed = one[1] * jnp.exp(one[0] - top) + other[1] * jnp.exp(other[0] - top)
    return jnp.stack([top, summed])


def summed_scores(scorer, query_len, owners):
    block_size = scorer.block_shape[0]
    if owners != 4:
        sent = scorer.first(owners - 1, block_size)
        parts = []
        for distance in range(owners - 1, -1, -1):
            ahead = distance - 1 if distance > 0 else None
            if distance < owners - 1:
                sent = scorer(distance, 0, block_size, ahead)
            elif ahead is not None:
                scorer(distance, 0, block_size, ahead)
            parts.append(exchange(sent, "gz", distance) if distance else sent)
        total = merge(parts, [0] * len(parts), block_size, query_len)
        return hypercube(total, "gy", jnp.add)
    early = block_size * 3 // 8
    late = block_size - early
    near_0 = exchange(scorer.first(3, early), "gz", 1)
    near_1 = exchange(scorer(3, early, late, 2), "gz", 1)
    far_0 = exchange(jnp.maximum(scorer(2, 0, early, 1), near_0), "gz", 2)
    beside_0 = exchange(scorer(1, 0, early, 0), "gz", 1)
    far_1 = exchange(jnp.maximum(scorer(2, early, late), near_1), "gz", 2)
    beside_1 = exchange(scorer(1, early, late), "gz", 1)
    own_0 = scorer(0, 0, early)
    own_1 = scorer(0, early, late)
    first = merge([own_0, beside_0, far_0], [0, 0, 0], early, query_len)
    first = hypercube(first, "gy", jnp.add)
    query_len, first = lax.optimization_barrier((query_len, first))
    second = merge([own_1, beside_1, far_1], [0, 0, 0], late, query_len)
    others = [exchange(second, "gy", distance) for distance in range(1, lax.axis_size("gy"))]
    second = functools.reduce(jnp.add, others, second)
    return jnp.concatenate([first, second])


def shards(queries, passages, passage_len, query_len):
    query_count, query_rows, width = queries.shape
    owners = lax.axis_size("gz")
    flat_queries = queries.reshape(query_count * query_rows, width)
    scorer = Scorer(flat_queries, passages, passage_len, owners)
    scores = summed_scores(scorer, query_len, owners)
    top = jnp.max(scores, axis=0)
    summed = jnp.sum(jnp.exp(scores - top[None]), axis=0)
    pair = hypercube(jnp.stack([top, summed]), "gx", join_pairs)
    others = [exchange(pair, "gz", distance) for distance in range(1, owners)]
    pair = functools.reduce(join_pairs, others, pair)
    return jnp.transpose(scores - (pair[0] + jnp.log(pair[1]))[None])


def solution(mesh):
    return jax.shard_map(
        shards,
        mesh=mesh,
        in_specs=(P(None, "gy", None), P("gx", "gz", None), P("gx"), P()),
        out_specs=P(None, ("gx", "gz")),
        check_vma=False,
    )
```
